32 devices in a mesh: grp: 4 (over y, core), fsdp: 2 (over x), tp: 4 (over z).
Axes of the slice: x: 2, y: 2, z: 4, core: 2. Of those that a mesh axis runs over, the one named last changes fastest.
Arguments:
- trained_weight: bfloat16 [28672, 4096], P(('fsdp', 'tp'), 'grp'), may hold values from -0.03125 to 0.03125
- hidden: bfloat16 [4, 256, 28672], P('grp', None, 'fsdp'), may hold values from -6 to 6
Outputs:
- served_weight: bfloat16 [28672, 4096], P('fsdp', 'tp')
- decoded: bfloat16 [4, 256, 4096], P('grp', None, 'tp')
The draws below stay inside these ranges and needn't reach their ends.
All inputs are finite; a program needn't handle non-finite values.
Results may differ from the reference program's by a relative error of at most 0.001.
Values may be sent and summed in bfloat16 or wider, within the bound.
No kernel may reach another device: no remote copies, remote signals or barrier semaphores. Data moves between devices by JAX's collectives and lax.ppermute only.
A program may use at most 128 MiB of HBM per device.

```python
import jax
import jax.numpy as jnp

D = 4096
FF = 28672
TOK = 256
GROUPS = 4


def steps_of(key, dims, split, least, top_value):
    level, own = 1.0, jax.random.fold_in(key, 6)
    for position, blocks in split:
        draws = jnp.exp(jax.random.uniform(jax.random.fold_in(own, position), (blocks,), jnp.float32, least / len(split), top_value / len(split)))
        level = level * jnp.repeat(draws, dims[position] // blocks).reshape([-1 if axis == position else 1 for axis in range(len(dims))])
    return level


def gaussian(own_key, shape, deviation, reach, cuts=(), dtype=jnp.bfloat16):
    level = steps_of(own_key, shape, cuts, -0.22, 0.18) if cuts else 1.0
    values = jax.random.normal(own_key, shape, jnp.float32) * deviation * level
    return jnp.minimum(jnp.maximum(values, -reach), reach).astype(dtype)


def setup_inputs(seed: int = 0) -> dict:
    seeds = jax.random.split(jax.random.key(seed), 3)
    return {
        "trained_weight": gaussian(seeds[0], (FF, D), FF ** -0.5, 0.03125, ((0, 8), (1, 4))),
        "hidden": gaussian(seeds[1], (GROUPS, TOK, FF), 1.0, 6.0, ((0, 4), (2, 2))),
    }


def reference(trained_weight, hidden):
    served_weight = trained_weight
    flat = hidden.reshape(GROUPS * TOK, FF)
    product = jnp.dot(flat, served_weight, preferred_element_type=jnp.float32)
    decoded = product.reshape(GROUPS, TOK, D).astype(jnp.bfloat16)
    return served_weight, decoded
```

```python
import jax
import jax.numpy as jnp
from jax import lax
from jax.sharding import PartitionSpec as P

CORES = 2
PIECES = 4


def general(trained_weight, hidden):
    groups = lax.axis_size("grp")
    blocks_tp = lax.axis_size("tp")
    rows_local = trained_weight.shape[0]
    hidden_rows = hidden[0]
    tokens_here = hidden_rows.shape[0]
    spread = lax.all_to_all(trained_weight, "grp", split_axis=0, concat_axis=1, tiled=True)
    sliced = lax.all_to_all(spread, "tp", split_axis=1, concat_axis=0, tiled=True)
    share = rows_local // groups
    columns = sliced.shape[1]
    pieces = sliced.reshape(blocks_tp, 1, share, columns)
    hidden_four = hidden_rows.reshape(tokens_here, blocks_tp, groups, share)
    piece = lax.all_gather(pieces, "grp", axis=1, tiled=True)
    running = jnp.einsum("btgr,tgrc->bc", hidden_four, piece, preferred_element_type=jnp.float32)
    served = piece.reshape(blocks_tp * groups * share, columns)
    total = lax.psum(running, "fsdp")
    return (served, total.astype(jnp.bfloat16)[None])


def fsdp_sum(value):
    size = lax.axis_size("fsdp")
    if size == 2:
        return value + lax.ppermute(value, "fsdp", [(0, 1), (1, 0)])
    return lax.psum(value, "fsdp")


def staged(trained_weight, hidden):
    groups = lax.axis_size("grp")
    blocks_tp = lax.axis_size("tp")
    sides = groups // CORES
    rows, columns = trained_weight.shape
    half = columns // sides
    width = half // PIECES
    hidden_rows = hidden[0]
    side = lax.axis_index("grp") // CORES
    core = lax.axis_index("grp") % CORES
    plane = lax.axis_index("tp")
    swap = [(i, (i + CORES) % groups) for i in range(groups)]
    sibling = [(i, i ^ 1) for i in range(groups)]

    def exchange(k):
        pairs = []
        for y in range(sides):
            for c in range(CORES):
                for z in range(blocks_tp):
                    source = (y * CORES + c) * blocks_tp + z
                    to_plane = CORES * ((z + k) % sides) + c
                    target = (y * CORES + z // sides) * blocks_tp + to_plane
                    pairs.append((source, target))
        return pairs

    routes = [exchange(k) for k in range(sides)]
    own_first = plane % sides == side
    near = side == 0
    pieces = range(PIECES)
    got, came, other, came_too, other_too, partial, total = ({} for _ in range(7))
    state = {"weight": trained_weight, "served": jnp.zeros((CORES, sides, rows, columns), trained_weight.dtype)}

    def cross(p):
        away = lax.dynamic_slice(state["weight"], (0, (1 - side) * half + p * width), (rows, width))
        got[p] = lax.ppermute(away, "grp", swap)

    def spread(p):
        keep = lax.dynamic_slice(state["weight"], (0, side * half + p * width), (rows, width))
        for k in range(sides):
            sent = jnp.where(own_first == (k == 0), keep, got[p])
            came[p, k] = lax.ppermute(sent, ("grp", "tp"), routes[k])
        del got[p]

    def back(p):
        for k in range(sides):
            other[p, k] = lax.ppermute(came[p, k], "grp", swap)

    def share_came(p):
        for k in range(sides):
            came_too[p, k] = lax.ppermute(came[p, k], "grp", sibling)

    def share_other(p):
        for k in range(sides):
            other_too[p, k] = lax.ppermute(other[p, k], "grp", sibling)

    def place(p, mine, theirs, where):
        served = state["served"]
        for k in range(sides):
            low = (plane // CORES + k) % sides
            a, b = mine.pop((p, k)), theirs.pop((p, k))
            for y in range(sides):
                block = jnp.where(near == (y == 0), a, b)
                served = lax.dynamic_update_slice(served, block[None, None], (where, low, 0, y * half + p * width))
        state["served"] = served

    def product(p):
        whole = state["served"].reshape(blocks_tp * rows, columns)
        for y in range(sides):
            block = whole[:, y * half + p * width : y * half + (p + 1) * width]
            partial[y, p] = jnp.dot(hidden_rows, block, preferred_element_type=jnp.float32)

    def reduce(p):
        for y in range(sides):
            total[y, p] = fsdp_sum(partial.pop((y, p))).astype(jnp.bfloat16)

    def settle(late=()):
        held = (state, got, came, other, came_too, other_too, partial, total)
        places = [(d, name) for d in held for name in sorted(d) if not any(d is of and name in names for of, names in late)]
        fresh = lax.optimization_barrier([d[name] for d, name in places])
        for (d, name), value in zip(places, fresh):
            d[name] = value

    cross(0)
    settle()
    for step in range(PIECES + 2):
        if step < PIECES:
            spread(step)
        for p in ((1, 2) if step == 0 else (step + 2,)):
            if p < PIECES:
                cross(p)
        if 0 <= step - 1 < PIECES:
            back(step - 1)
            share_came(step - 1)
        if 0 <= step - 2 < PIECES:
            share_other(step - 2)
            place(step - 2, came, other, core)
            place(step - 2, came_too, other_too, 1 - core)
            product(step - 2)
            reduce(step - 2)
        if step < PIECES:
            settle(((came, [(step, 1)]), (other, [(step - 1, 1)])))
    decoded = [total[y, p] for y in range(sides) for p in pieces]
    return (state["served"].reshape(blocks_tp * rows, columns), jnp.concatenate(decoded, axis=1)[None])


def solution(mesh):
    groups, blocks_tp = mesh.shape["grp"], mesh.shape["tp"]
    paired = groups == blocks_tp == CORES * CORES
    return jax.shard_map(
        staged if paired else general,
        mesh=mesh,
        in_specs=(P(("fsdp", "tp"), "grp"), P("grp", None, "fsdp")),
        out_specs=(P("fsdp", "tp"), P("grp", None, "tp")),
        check_vma=False,
    )
```
